32 devices in a mesh: groups: 2 (over y), bank: 4 (over x, core), tensor: 4 (over z).
Axes of the slice: x: 2, y: 2, z: 4, core: 2. Of those that a mesh axis runs over, the one named last changes fastest.
Arguments:
- latest_activations: bfloat16 [64, 8192], P(('groups', 'bank'), 'tensor'), parts along dimension 0, may hold values from -6 to 6
- layer_normalizer_gains_table: bfloat16 [8192], replicated, may hold values from 0.5 to 1.5
- asker_projection: bfloat16 [8192, 8192], P('bank', 'tensor'), may hold values from -0.0625 to 0.0625
- memory_projection_stack: bfloat16 [2, 8192, 1024], P(None, 'bank', 'tensor'), may hold values from -0.0625 to 0.0625
- narrowing_factors: bfloat16 [128, 48, 8192], P('bank', None, 'tensor'), may hold values from -0.0625 to 0.0625
- widening_factors_asker: bfloat16 [128, 16, 8192], P('bank', None, 'tensor'), may hold values from -1.5 to 1.5
- widening_factors_memory: bfloat16 [128, 2, 16, 1024], P('bank', None, None, 'tensor'), may hold values from -1.5 to 1.5
- tweak_for_stream: int32 [64], P(('groups', 'bank')), parts along dimension 0, may hold values from 0 to 127
- stream_offsets: int32 [64], P(('groups', 'bank')), parts along dimension 0, may hold values from 2 to 1024
- saved_rotated_addresses: bfloat16 [64, 1024, 8, 128], P(('groups', 'bank'), None, 'tensor'), parts along dimension 0, may hold values from -1200 to 1200
- saved_contents: bfloat16 [64, 1024, 8, 128], P(('groups', 'bank'), None, 'tensor'), parts along dimension 0, may hold values from -6 to 6
Outputs:
- attention: bfloat16 [64, 8192], P(('groups', 'bank'), 'tensor'), parts along dimension 0
The draws below stay inside these ranges and needn't reach their ends.
There are 2 independent parts, one for each index of `groups`. The reference program is written for one: setup_inputs(seed, part) draws one part's arguments, and reference() takes and returns one part's arrays. A program takes and returns all parts, laid end to end along the dimension named above; an argument that names none is the same for every part. Nothing has to cross between parts.
All inputs are finite; a program needn't handle non-finite values.
Results may differ from the reference program's by a relative error of at most 0.0095.
The reference program's roundings to bfloat16 on the way (of `normed`, `inner_low` and `weights`) count: a program that leaves them out, or rounds other values in their place, can miss the bound.
Values may be sent and summed in bfloat16 or wider, within the bound.
No kernel may reach another device: no remote copies, remote signals or barrier semaphores. Data moves between devices by JAX's collectives and lax.ppermute only.
A program may use at most 64 MiB of HBM per device.

```python
import math
import jax
import jax.numpy as jnp
import numpy as np
from jax import lax

MODEL_BREADTH = 8192
ASKER_LANES = 64
MEMORY_LANES = 8
SUBSPACE_BREADTH = 128
NARROW_ORDER = 16
TWEAK_POOL = 128
STREAM_TOTAL = 32
CTX = 1024


def draw_saved_rotated_addresses(key, part):
    first_key = jax.random.fold_in(key, 11)
    values = 0.35 * jnp.clip(jax.random.normal(first_key, (STREAM_TOTAL, CTX, MEMORY_LANES, SUBSPACE_BREADTH), jnp.float32), -5.0, 5.0)
    return values.astype(jnp.bfloat16)


def with_ends(array, own_key, low, largest):
    dims = array.shape
    place = [jax.random.randint(jax.random.fold_in(own_key, axis), (), 0, dims[axis]) for axis in range(len(dims))]
    array = array.at[tuple(place)].set(low)
    longest = dims.index(max(dims))
    place[longest] = (place[longest] + 1) % dims[longest]
    return array.at[tuple(place)].set(largest)


def block_scale(own_key, dims, shards, smallest, high):
    def one(position, blocks):
        draws = jax.random.uniform(jax.random.fold_in(jax.random.fold_in(own_key, 6), position), (blocks,), jnp.float32, smallest / len(shards), high / len(shards))
        return jnp.repeat(jnp.exp(draws), dims[position] // blocks).reshape((-1,) + (1,) * (len(dims) - position - 1))

    factor_of = one(*shards[0])
    for cut in shards[1:]:
        factor_of = factor_of * one(*cut)
    return factor_of


def rank_bounds(count, slope):
    loads = [(1 << 20) // math.isqrt(standing ** slope) + 1 for standing in range(1, count + 1)]
    width = 1 + sum(loads) // (1 << 30)
    return np.cumsum(np.array([max(1, weight // width) for weight in loads]))


def skewed_ids(stream_key, shape, count, skew):
    listing = rank_bounds(count, skew)
    pick = jax.random.randint(jax.random.fold_in(stream_key, 1), shape, 0, int(listing[count - 1]))
    grade = jnp.searchsorted(jnp.asarray(listing, jnp.int32), pick, side="right")
    return jax.random.permutation(jax.random.fold_in(stream_key, 2), count)[grade].astype(jnp.int32)


def noise(rng, extent, spread, limit, split=(), kind=jnp.bfloat16):
    loudness = block_scale(rng, extent, split, -0.22, 0.18) if split else 1.0
    values = jax.random.normal(rng, extent, jnp.float32) * spread * loudness
    return jnp.minimum(jnp.maximum(values, -limit), limit).astype(kind)


def setup_inputs(seed: int = 0, part: int = 0) -> dict:
    streams_of = jax.random.split(jax.random.key(seed), 12)
    own_keys = jax.random.split(jax.random.fold_in(streams_of[11], part), 12)
    return {
        "latest_activations": noise(own_keys[0], (STREAM_TOTAL, MODEL_BREADTH), 1.0, 6.0, ((0, 4), (1, 4))),
        "layer_normalizer_gains_table": jnp.clip(1.0 + 0.1 * jax.random.normal(streams_of[1], (MODEL_BREADTH,), jnp.float32), 0.5, 1.5).astype(jnp.bfloat16),
        "asker_projection": noise(streams_of[2], (MODEL_BREADTH, ASKER_LANES * SUBSPACE_BREADTH), MODEL_BREADTH ** -0.5, 0.0625, ((0, 4), (1, 4))),
        "memory_projection_stack": noise(streams_of[3], (2, MODEL_BREADTH, MEMORY_LANES * SUBSPACE_BREADTH), MODEL_BREADTH ** -0.5, 0.0625, ((1, 4), (2, 4))),
        "narrowing_factors": noise(streams_of[4], (TWEAK_POOL, 3 * NARROW_ORDER, MODEL_BREADTH), MODEL_BREADTH ** -0.5, 0.0625, ((0, 4), (2, 4))),
        "widening_factors_asker": noise(streams_of[5], (TWEAK_POOL, NARROW_ORDER, ASKER_LANES * SUBSPACE_BREADTH), NARROW_ORDER ** -0.5, 1.5, ((0, 4), (2, 4))),
        "widening_factors_memory": noise(streams_of[6], (TWEAK_POOL, 2, NARROW_ORDER, MEMORY_LANES * SUBSPACE_BREADTH), NARROW_ORDER ** -0.5, 1.5, ((0, 4), (3, 4))),
        "tweak_for_stream": with_ends(skewed_ids(own_keys[7], (STREAM_TOTAL,), TWEAK_POOL, 2), jax.random.fold_in(own_keys[7], 3), 0, TWEAK_POOL - 1).astype(jnp.int32),
        "stream_offsets": with_ends(jax.random.randint(own_keys[8], (STREAM_TOTAL,), 2, CTX + 1), jax.random.fold_in(own_keys[8], 1), 2, CTX).astype(jnp.int32),
        "saved_rotated_addresses": draw_saved_rotated_addresses(jax.random.fold_in(jax.random.fold_in(streams_of[11], part), 71), part),
        "saved_contents": noise(own_keys[10], (STREAM_TOTAL, CTX, MEMORY_LANES, SUBSPACE_BREADTH), 1.0, 6.0, ((0, 4), (2, 4))),
    }


rope_base = 500000.0
tweak_strength = 2.0
epsilon = 1e-05

def rotate(values, positions):
    half_dim = values.shape[-1] // 2
    freqs = rope_base ** (-(jnp.arange(half_dim, dtype=jnp.float32) * 2.0) / values.shape[-1])
    angles = positions.astype(jnp.float32)[:, None] * freqs[None, :]
    cosine = jnp.cos(angles)[:, None, :]
    sine_part = jnp.sin(angles)[:, None, :]
    front_half = values[..., :half_dim]
    back_half = values[..., half_dim:]
    return jnp.concatenate([front_half * cosine - back_half * sine_part, back_half * cosine + front_half * sine_part], axis=-1)

def attend(probe_vectors, current_lookup_vectors, values_new, cache_keys, cache_values, stream_offsets):
    reciprocal_sqrt_dim = 1.0 / math.sqrt(probe_vectors.shape[-1])
    scores = jnp.einsum('bkgd,bpkd->bkgp', probe_vectors.astype(jnp.float32), cache_keys.astype(jnp.float32)) * reciprocal_sqrt_dim
    self_logit = jnp.einsum('atcj,atj->atc', probe_vectors.astype(jnp.float32), current_lookup_vectors.astype(jnp.float32)) * reciprocal_sqrt_dim
    positions = lax.broadcasted_iota(jnp.int32, scores.shape, 3)
    live_mask = positions < stream_offsets.astype(jnp.int32)[:, None, None, None]
    peak_score = jnp.maximum(lax.optimization_barrier(jnp.max(jnp.where(live_mask, scores, -jnp.inf), axis=-1)), self_logit)
    expo = jnp.where(live_mask, jnp.exp(scores - peak_score[..., None]), 0.0)
    own_expo = jnp.exp(self_logit - peak_score)
    total = lax.optimization_barrier(jnp.sum(expo, axis=-1)) + own_expo
    weights = (expo / total[..., None]).astype(jnp.bfloat16)
    own_weight = (own_expo / total).astype(jnp.bfloat16)
    mixed = jnp.einsum('bkgp,bpkd->bkgd', weights.astype(jnp.float32), cache_values.astype(jnp.float32))
    return mixed + own_weight.astype(jnp.float32)[..., None] * values_new.astype(jnp.float32)[:, :, None, :]

def reference(latest_activations, layer_normalizer_gains_table, asker_projection, memory_projection_stack, narrowing_factors, widening_factors_asker, widening_factors_memory, tweak_for_stream, stream_offsets, saved_rotated_addresses, saved_contents):
    tok_float = latest_activations.astype(jnp.float32)
    mean_square = lax.optimization_barrier(jnp.mean(tok_float * tok_float, axis=1, keepdims=True))
    normed = (tok_float * lax.rsqrt(mean_square + epsilon) * layer_normalizer_gains_table.astype(jnp.float32)[None, :]).astype(jnp.bfloat16)
    probe_vector_frozen = jnp.dot(normed, asker_projection, preferred_element_type=jnp.float32)
    lookup_vector_frozen = jnp.dot(normed, memory_projection_stack[0], preferred_element_type=jnp.float32)
    payload_vector_frozen = jnp.dot(normed, memory_projection_stack[1], preferred_element_type=jnp.float32)
    picked_narrowing = jnp.take(narrowing_factors, tweak_for_stream, axis=0)
    inner = jnp.einsum('brd,bd->br', picked_narrowing.astype(jnp.float32), normed.astype(jnp.float32))
    inner_low = inner.astype(jnp.bfloat16).astype(jnp.float32)
    picked_widening_asker = jnp.take(widening_factors_asker, tweak_for_stream, axis=0).astype(jnp.float32)
    picked_widening_memory = jnp.take(widening_factors_memory, tweak_for_stream, axis=0).astype(jnp.float32)
    probe_correction = jnp.einsum('br,bro->bo', inner_low[:, :NARROW_ORDER], picked_widening_asker)
    lookup_correction = jnp.einsum('br,bro->bo', inner_low[:, NARROW_ORDER:2 * NARROW_ORDER], picked_widening_memory[:, 0])
    payload_correction = jnp.einsum('br,bro->bo', inner_low[:, 2 * NARROW_ORDER:3 * NARROW_ORDER], picked_widening_memory[:, 1])
    probe_vector_final = probe_vector_frozen + tweak_strength * probe_correction
    lookup_vector_final = lookup_vector_frozen + tweak_strength * lookup_correction
    payload_vector_final = payload_vector_frozen + tweak_strength * payload_correction
    q_rot = rotate(probe_vector_final.reshape(STREAM_TOTAL, ASKER_LANES, SUBSPACE_BREADTH), stream_offsets).astype(jnp.bfloat16)
    k_new = rotate(lookup_vector_final.reshape(STREAM_TOTAL, MEMORY_LANES, SUBSPACE_BREADTH), stream_offsets).astype(jnp.bfloat16)
    v_new = payload_vector_final.reshape(STREAM_TOTAL, MEMORY_LANES, SUBSPACE_BREADTH).astype(jnp.bfloat16)
    probe_vectors = q_rot.reshape(STREAM_TOTAL, MEMORY_LANES, ASKER_LANES // MEMORY_LANES, SUBSPACE_BREADTH)

    def per_sequence(packed):
        query_one, key_one, value_one, cache_key_one, cache_value_one, length_one = packed
        return attend(query_one[None], key_one[None], value_one[None], cache_key_one[None], cache_value_one[None], length_one[None])[0]
    mixed = lax.map(per_sequence, (probe_vectors, k_new, v_new, saved_rotated_addresses, saved_contents, stream_offsets))
    return mixed.reshape(STREAM_TOTAL, ASKER_LANES * SUBSPACE_BREADTH).astype(jnp.bfloat16)
```

```python
import math

import jax
import jax.numpy as jnp
from jax import lax
from jax.experimental import pallas as pl
from jax.experimental.pallas import tpu as pltpu
from jax.sharding import PartitionSpec as P


rope_base = 500000.0
tweak_strength = 2.0
epsilon = 1e-05


def rotate(values, positions):
    half_dim = values.shape[-1] // 2
    freqs = rope_base ** (-(jnp.arange(half_dim, dtype=jnp.float32) * 2.0) / values.shape[-1])
    angles = positions.astype(jnp.float32)[:, None] * freqs[None, :]
    cosine = jnp.cos(angles)[:, None, :]
    sine_part = jnp.sin(angles)[:, None, :]
    front_half = values[..., :half_dim]
    back_half = values[..., half_dim:]
    return jnp.concatenate(
        [front_half * cosine - back_half * sine_part, back_half * cosine + front_half * sine_part],
        axis=-1,
    )


def attend_local(
    probe_vectors, current_lookup_vectors, values_new, cache_keys, cache_values, stream_offsets
):
    reciprocal_sqrt_dim = 1.0 / math.sqrt(probe_vectors.shape[-1])
    scores = (
        jnp.einsum("bkgd,bpkd->bkgp", probe_vectors, cache_keys, preferred_element_type=jnp.float32)
        * reciprocal_sqrt_dim
    )
    self_logit = (
        jnp.einsum(
            "atcj,atj->atc",
            probe_vectors,
            current_lookup_vectors,
            preferred_element_type=jnp.float32,
        )
        * reciprocal_sqrt_dim
    )
    positions = lax.broadcasted_iota(jnp.int32, scores.shape, 3)
    live_mask = positions < stream_offsets[:, None, None, None]
    peak_score = jnp.maximum(jnp.max(jnp.where(live_mask, scores, -jnp.inf), axis=-1), self_logit)
    expo = jnp.where(live_mask, jnp.exp(scores - peak_score[..., None]), 0.0)
    own_expo = jnp.exp(self_logit - peak_score)
    total = jnp.sum(expo, axis=-1) + own_expo
    weights = (expo / total[..., None]).astype(jnp.bfloat16)
    own_weight = (own_expo / total).astype(jnp.bfloat16)
    mixed = jnp.einsum("bkgp,bpkd->bkgd", weights, cache_values, preferred_element_type=jnp.float32)
    return (
        mixed
        + own_weight.astype(jnp.float32)[..., None] * values_new.astype(jnp.float32)[:, :, None, :]
    )


def ring(size, shift):
    return [(place, (place + shift) % size) for place in range(size)]


def relative_blocks(piece, axis, size):
    return [piece] + [lax.ppermute(piece, axis, ring(size, shift)) for shift in range(1, size)]


def swapped(rows, n_bank, n_tensor, bank_index):
    fold = n_bank // n_tensor
    width = rows.shape[1] // fold
    if fold > 1:
        rows = lax.dynamic_slice_in_dim(rows, (bank_index // n_tensor) * width, width, 1)
    pairs = [
        (b * n_tensor + t, (t * fold + b // n_tensor) * n_tensor + b % n_tensor)
        for b in range(n_bank)
        for t in range(n_tensor)
    ]
    return lax.ppermute(rows, ("bank", "tensor"), pairs)


def digits_of(ids):
    return jnp.stack([ids // 65536, (ids // 256) % 256, ids % 256], axis=1).astype(jnp.bfloat16)


def ids_from(digits):
    whole = digits.astype(jnp.float32)
    return (whole[:, 0] * 65536.0 + whole[:, 1] * 256.0 + whole[:, 2]).astype(jnp.int32)


def narrow_body(first_ref, ids_ref, row_ids_ref, rows_ref, bank_ref, out_ref, buffer, wanted, sems):
    own = bank_ref.shape[0]
    first = first_ref[0]

    @pl.loop(0, own)
    def _(slot):
        wanted[slot] = 0

    @pl.loop(0, ids_ref.shape[0])
    def _(row):
        slot = ids_ref[row] - first

        @pl.when((slot >= 0) & (slot < own))
        def _():
            place = jnp.clip(slot, 0, own - 1)

            @pl.when(wanted[place] == 0)
            def _():
                wanted[place] = 1
                pltpu.make_async_copy(bank_ref.at[place], buffer.at[place], sems.at[place]).start()

    out_ref[...] = jnp.zeros(out_ref.shape, jnp.float32)

    @pl.loop(0, own)
    def _(slot):
        @pl.when(wanted[slot] == 1)
        def _():
            pltpu.make_async_copy(bank_ref.at[slot], buffer.at[slot], sems.at[slot]).wait()
            low = lax.dot_general(
                buffer[slot],
                rows_ref[...],
                (((1,), (1,)), ((), ())),
                preferred_element_type=jnp.float32,
            )
            out_ref[...] = jnp.where(row_ids_ref[...] == slot + first, low, out_ref[...])


def narrow(first, ids, rows, bank):
    own, ranks, width = bank.shape
    return pl.pallas_call(
        narrow_body,
        out_shape=jax.ShapeDtypeStruct((ranks, rows.shape[0]), jnp.float32),
        in_specs=[
            pl.BlockSpec(memory_space=pltpu.SMEM),
            pl.BlockSpec(memory_space=pltpu.SMEM),
            pl.BlockSpec(memory_space=pltpu.VMEM),
            pl.BlockSpec(memory_space=pltpu.VMEM),
            pl.BlockSpec(memory_space=pl.ANY),
        ],
        out_specs=pl.BlockSpec(memory_space=pltpu.VMEM),
        scratch_shapes=[
            pltpu.VMEM((own, ranks, width), bank.dtype),
            pltpu.SMEM((own,), jnp.int32),
            pltpu.SemaphoreType.DMA((own,)),
        ],
        name="narrow",
    )(first, ids, ids[None, :], rows, bank)


CHUNKS = 4


def base_body(turn_ref, rows_ref, ask_ref, mem_ref, out_ref, ask_buf, mem_buf, turned, sems):
    depth = ask_ref.shape[0] // CHUNKS
    span = ask_ref.shape[1]
    side = mem_ref.shape[2]

    def copies(step):
        cut = pl.ds(step * depth, depth)
        return (
            pltpu.make_async_copy(ask_ref.at[cut], ask_buf.at[cut], sems.at[step, 0]),
            pltpu.make_async_copy(mem_ref.at[0, cut], mem_buf.at[0, cut], sems.at[step, 1]),
            pltpu.make_async_copy(mem_ref.at[1, cut], mem_buf.at[1, cut], sems.at[step, 2]),
        )

    for step in range(CHUNKS):
        for copy in copies(step):
            copy.start()
    count = rows_ref.shape[0]
    blocks = count // 8
    for block in range(blocks):
        start = pl.multiple_of(((turn_ref[0] + block) % blocks) * 8, 8)
        turned[pl.ds(block * 8, 8), :] = rows_ref[pl.ds(start, 8), :]
    for step in range(CHUNKS):
        for copy in copies(step):
            copy.wait()
        cut = pl.ds(step * depth, depth)
        left = turned[:, cut]

        def add(place, width, weights):
            value = jnp.dot(left, weights, preferred_element_type=jnp.float32)
            if step:
                value = value + out_ref[:, pl.ds(place, width)]
            out_ref[:, pl.ds(place, width)] = value

        add(0, span, ask_buf[cut, :])
        add(span, side, mem_buf[0, cut, :])
        add(span + side, side, mem_buf[1, cut, :])


def base_product(turn, rows, ask, mem):
    return pl.pallas_call(
        base_body,
        out_shape=jax.ShapeDtypeStruct((rows.shape[0], ask.shape[1] + 2 * mem.shape[2]), jnp.float32),
        in_specs=[
            pl.BlockSpec(memory_space=pltpu.SMEM),
            pl.BlockSpec(memory_space=pltpu.VMEM),
            pl.BlockSpec(memory_space=pl.ANY),
            pl.BlockSpec(memory_space=pl.ANY),
        ],
        out_specs=pl.BlockSpec(memory_space=pltpu.VMEM),
        scratch_shapes=[
            pltpu.VMEM(ask.shape, ask.dtype),
            pltpu.VMEM(mem.shape, mem.dtype),
            pltpu.VMEM(rows.shape, rows.dtype),
            pltpu.SemaphoreType.DMA((CHUNKS, 3)),
        ],
        name="base",
    )(turn, rows, ask, mem)


def shards(
    latest_activations,
    layer_normalizer_gains_table,
    asker_projection,
    memory_projection_stack,
    narrowing_factors,
    widening_factors_asker,
    widening_factors_memory,
    tweak_for_stream,
    stream_offsets,
    saved_rotated_addresses,
    saved_contents,
):
    n_bank = lax.axis_size("bank")
    n_tensor = lax.axis_size("tensor")
    bank_index = lax.axis_index("bank")
    tensor_index = lax.axis_index("tensor")
    row_count, piece_tensor = latest_activations.shape
    model_width = layer_normalizer_gains_table.shape[0]
    fold = n_bank // n_tensor

    own_float = latest_activations.astype(jnp.float32)
    part_square = jnp.sum(own_float * own_float, axis=1)
    square = sum(relative_blocks(part_square, "tensor", n_tensor))[:, None]
    tensor_gain = lax.dynamic_slice_in_dim(
        layer_normalizer_gains_table, tensor_index * piece_tensor, piece_tensor, 0
    )
    normed = (
        own_float
        * lax.rsqrt(square / model_width + epsilon)
        * tensor_gain.astype(jnp.float32)[None, :]
    ).astype(jnp.bfloat16)
    note = jnp.pad(digits_of(tweak_for_stream), ((0, 0), (0, 125)))
    package = jnp.concatenate([normed, note], axis=1)
    packages = jnp.concatenate(relative_blocks(package, "bank", n_bank), axis=0)
    hidden_after_rmsnorm = packages[:, :piece_tensor]
    all_ids = ids_from(packages[:, piece_tensor : piece_tensor + 3])
    base_rows = swapped(hidden_after_rmsnorm, n_bank, n_tensor, bank_index)
    source_bank = (bank_index % fold) * n_tensor + tensor_index
    turn = ((source_bank - bank_index) % n_bank) * (row_count // 8)

    sequences_on_device = narrowing_factors.shape[0]
    low_dim_extent = widening_factors_asker.shape[1]
    owned_ids = bank_index * sequences_on_device + jnp.arange(sequences_on_device, dtype=jnp.int32)
    picked = all_ids[None, :] == owned_ids[:, None]
    first = (bank_index * sequences_on_device).astype(jnp.int32)[None]
    inner_part = narrow(first, all_ids, hidden_after_rmsnorm, narrowing_factors)
    inner_sum = sum(relative_blocks(inner_part, "tensor", n_tensor))
    inner_low = inner_sum.astype(jnp.bfloat16)
    pick_low = picked.astype(jnp.bfloat16)
    base_part = base_product(
        turn.astype(jnp.int32)[None], base_rows, asker_projection, memory_projection_stack
    )

    def spread(rank_block):
        expanded = pick_low[:, None, :] * rank_block[None, :, :]
        return expanded.reshape(sequences_on_device * low_dim_extent, rank_block.shape[1])

    probe_proj_span = asker_projection.shape[1]
    shared_proj_span = memory_projection_stack.shape[2]
    probe_correction = jnp.einsum(
        "cs,co->so",
        spread(inner_low[0:low_dim_extent]),
        widening_factors_asker.reshape(sequences_on_device * low_dim_extent, probe_proj_span),
        preferred_element_type=jnp.float32,
    )
    lookup_correction = jnp.einsum(
        "cs,co->so",
        spread(inner_low[low_dim_extent : 2 * low_dim_extent]),
        widening_factors_memory[:, 0].reshape(
            sequences_on_device * low_dim_extent, shared_proj_span
        ),
        preferred_element_type=jnp.float32,
    )
    payload_correction = jnp.einsum(
        "cs,co->so",
        spread(inner_low[2 * low_dim_extent : 3 * low_dim_extent]),
        widening_factors_memory[:, 1].reshape(
            sequences_on_device * low_dim_extent, shared_proj_span
        ),
        preferred_element_type=jnp.float32,
    )
    share = base_part + tweak_strength * jnp.concatenate(
        [probe_correction, lookup_correction, payload_correction], axis=1
    )
    accumulated_total = share[:row_count]
    for r in range(1, n_bank):
        accumulated_total = accumulated_total + lax.ppermute(
            share[r * row_count : (r + 1) * row_count], "bank", ring(n_bank, -r)
        )
    head_dim = saved_rotated_addresses.shape[3]
    kv_heads = saved_rotated_addresses.shape[2]
    q_heads = probe_proj_span // head_dim
    query_part = accumulated_total[:, 0:probe_proj_span].reshape(row_count, q_heads, head_dim)
    key_part = accumulated_total[:, probe_proj_span : probe_proj_span + shared_proj_span].reshape(
        row_count, kv_heads, head_dim
    )
    value_part = accumulated_total[
        :, probe_proj_span + shared_proj_span : probe_proj_span + 2 * shared_proj_span
    ].reshape(row_count, kv_heads, head_dim)
    q_rot = rotate(query_part, stream_offsets).astype(jnp.bfloat16)
    k_new = rotate(key_part, stream_offsets).astype(jnp.bfloat16)
    v_new = value_part.astype(jnp.bfloat16)
    probe_vectors = q_rot.reshape(row_count, kv_heads, q_heads // kv_heads, head_dim)
    mixed = attend_local(
        probe_vectors, k_new, v_new, saved_rotated_addresses, saved_contents, stream_offsets
    )
    return mixed.reshape(row_count, probe_proj_span).astype(jnp.bfloat16)


def solution(mesh):
    placed = (
        P(("groups", "bank"), "tensor"),
        P(),
        P("bank", "tensor"),
        P(None, "bank", "tensor"),
        P("bank", None, "tensor"),
        P("bank", None, "tensor"),
        P("bank", None, None, "tensor"),
        P(("groups", "bank")),
        P(("groups", "bank")),
        P(("groups", "bank"), None, "tensor", None),
        P(("groups", "bank"), None, "tensor", None),
    )

    return jax.shard_map(
        shards,
        mesh=mesh,
        in_specs=placed,
        out_specs=P(("groups", "bank"), "tensor"),
        check_vma=False,
    )
```

```python
import math

import jax
import jax.numpy as jnp
from jax import lax
from jax.experimental import pallas as pl
from jax.experimental.pallas import tpu as pltpu
from jax.sharding import PartitionSpec as P


rope_base = 500000.0
tweak_strength = 2.0
epsilon = 1e-05


def rotate(values, positions):
    half_dim = values.shape[-1] // 2
    freqs = rope_base ** (-(jnp.arange(half_dim, dtype=jnp.float32) * 2.0) / values.shape[-1])
    angles = positions.astype(jnp.float32)[:, None] * freqs[None, :]
    cosine = jnp.cos(angles)[:, None, :]
    sine_part = jnp.sin(angles)[:, None, :]
    front_half = values[..., :half_dim]
    back_half = values[..., half_dim:]
    return jnp.concatenate(
        [front_half * cosine - back_half * sine_part, back_half * cosine + front_half * sine_part],
        axis=-1,
    )


def attend_local(
    probe_vectors, current_lookup_vectors, values_new, cache_keys, cache_values, stream_offsets
):
    reciprocal_sqrt_dim = 1.0 / math.sqrt(probe_vectors.shape[-1])
    scores = (
        jnp.einsum("bkgd,bpkd->bkgp", probe_vectors, cache_keys, preferred_element_type=jnp.float32)
        * reciprocal_sqrt_dim
    )
    self_logit = (
        jnp.einsum(
            "atcj,atj->atc",
            probe_vectors,
            current_lookup_vectors,
            preferred_element_type=jnp.float32,
        )
        * reciprocal_sqrt_dim
    )
    positions = lax.broadcasted_iota(jnp.int32, scores.shape, 3)
    live_mask = positions < stream_offsets[:, None, None, None]
    peak_score = jnp.maximum(jnp.max(jnp.where(live_mask, scores, -jnp.inf), axis=-1), self_logit)
    expo = jnp.where(live_mask, jnp.exp(scores - peak_score[..., None]), 0.0)
    own_expo = jnp.exp(self_logit - peak_score)
    total = jnp.sum(expo, axis=-1) + own_expo
    weights = (expo / total[..., None]).astype(jnp.bfloat16)
    own_weight = (own_expo / total).astype(jnp.bfloat16)
    mixed = jnp.einsum("bkgp,bpkd->bkgd", weights, cache_values, preferred_element_type=jnp.float32)
    return (
        mixed
        + own_weight.astype(jnp.float32)[..., None] * values_new.astype(jnp.float32)[:, :, None, :]
    )


def ring(size, shift):
    return [(place, (place + shift) % size) for place in range(size)]


def relative_blocks(piece, axis, size):
    return [piece] + [lax.ppermute(piece, axis, ring(size, shift)) for shift in range(1, size)]


def swapped(rows, n_bank, n_tensor, bank_index):
    fold = n_bank // n_tensor
    width = rows.shape[1] // fold
    if fold > 1:
        rows = lax.dynamic_slice_in_dim(rows, (bank_index // n_tensor) * width, width, 1)
    pairs = [
        (b * n_tensor + t, (t * fold + b // n_tensor) * n_tensor + b % n_tensor)
        for b in range(n_bank)
        for t in range(n_tensor)
    ]
    return lax.ppermute(rows, ("bank", "tensor"), pairs)


def digits_of(ids):
    return jnp.stack([ids // 65536, (ids // 256) % 256, ids % 256], axis=1).astype(jnp.bfloat16)


def ids_from(digits):
    whole = digits.astype(jnp.float32)
    return (whole[:, 0] * 65536.0 + whole[:, 1] * 256.0 + whole[:, 2]).astype(jnp.int32)


GROUP = 8


def narrow_body(
    first_ref,
    ids_ref,
    row_ids_ref,
    rows_ref,
    bank_ref,
    ask_ref,
    mem_ref,
    out_ref,
    ask_out,
    mem_out,
    buffer,
    wanted,
    names,
    sems,
    staged,
):
    own, ranks, _ = bank_ref.shape
    first = first_ref[0]

    @pl.loop(0, names.shape[0])
    def _(slot):
        wanted[slot] = 0
        names[slot] = -1

    def fetch(slot, place):
        cut = pl.ds(pl.multiple_of(place * ranks, ranks), ranks)
        return pltpu.make_async_copy(bank_ref.at[slot], buffer.at[cut], sems.at[place])

    def look(row, count):
        slot = ids_ref[row] - first
        mine = (slot >= 0) & (slot < own)
        local = jnp.clip(slot, 0, own - 1)
        fresh = mine & (wanted[local] == 0)

        @pl.when(fresh)
        def _():
            wanted[local] = 1
            names[count] = local + first
            fetch(local, count).start()

        return count + fresh.astype(jnp.int32)

    count = lax.fori_loop(0, ids_ref.shape[0], look, jnp.int32(0))
    copies = (
        pltpu.make_async_copy(ask_ref, ask_out, staged.at[0]),
        pltpu.make_async_copy(mem_ref, mem_out, staged.at[1]),
    )
    for copy in copies:
        copy.start()
    out_ref[...] = jnp.zeros(out_ref.shape, jnp.float32)

    @pl.loop(0, pl.cdiv(count, GROUP))
    def _(group):
        for member in range(GROUP):
            place = group * GROUP + member

            @pl.when(place < count)
            def _():
                fetch(0, place).wait()

        cut = pl.ds(pl.multiple_of(group * (GROUP * ranks), GROUP * ranks), GROUP * ranks)
        low = lax.dot_general(
            buffer[cut, :],
            rows_ref[...],
            (((1,), (1,)), ((), ())),
            preferred_element_type=jnp.float32,
        )
        total = out_ref[...]
        for member in range(GROUP):
            total = jnp.where(
                row_ids_ref[...] == names[group * GROUP + member],
                low[member * ranks : (member + 1) * ranks],
                total,
            )
        out_ref[...] = total

    for copy in copies:
        copy.wait()


def narrow(first, ids, rows, bank, ask, mem):
    own, ranks, width = bank.shape
    room = (own + GROUP - 1) // GROUP * GROUP
    bank, ask, mem = (
        pltpu.with_memory_space_constraint(held, pltpu.HBM) for held in (bank, ask, mem)
    )
    return pl.pallas_call(
        narrow_body,
        out_shape=(
            jax.ShapeDtypeStruct((ranks, rows.shape[0]), jnp.float32),
            pltpu.VMEM(ask.shape, ask.dtype),
            pltpu.VMEM(mem.shape, mem.dtype),
        ),
        in_specs=[
            pl.BlockSpec(memory_space=pltpu.SMEM),
            pl.BlockSpec(memory_space=pltpu.SMEM),
            pl.BlockSpec(memory_space=pltpu.VMEM),
            pl.BlockSpec(memory_space=pltpu.VMEM),
            pl.BlockSpec(memory_space=pltpu.HBM),
            pl.BlockSpec(memory_space=pltpu.HBM),
            pl.BlockSpec(memory_space=pltpu.HBM),
        ],
        out_specs=(pl.BlockSpec(memory_space=pltpu.VMEM),) * 3,
        scratch_shapes=[
            pltpu.VMEM((room * ranks, width), bank.dtype),
            pltpu.SMEM((room,), jnp.int32),
            pltpu.SMEM((room,), jnp.int32),
            pltpu.SemaphoreType.DMA((room,)),
            pltpu.SemaphoreType.DMA((2,)),
        ],
        compiler_params=pltpu.CompilerParams(vmem_limit_bytes=32 * 2**20),
        name="narrow",
    )(first, ids, ids[None, :], rows, bank, ask, mem)


def base_body(turn_ref, rows_ref, ask_ref, mem_ref, out_ref, turned):
    span = ask_ref.shape[1]
    side = mem_ref.shape[2]
    blocks = rows_ref.shape[0] // 8
    for block in range(blocks):
        start = pl.multiple_of(((turn_ref[0] + block) % blocks) * 8, 8)
        turned[pl.ds(block * 8, 8), :] = rows_ref[pl.ds(start, 8), :]
    left = turned[...]
    out_ref[:, pl.ds(0, span)] = jnp.dot(left, ask_ref[...], preferred_element_type=jnp.float32)
    for place in range(2):
        out_ref[:, pl.ds(span + place * side, side)] = jnp.dot(
            left, mem_ref[place], preferred_element_type=jnp.float32
        )


def base_product(turn, rows, ask, mem):
    return pl.pallas_call(
        base_body,
        out_shape=jax.ShapeDtypeStruct((rows.shape[0], ask.shape[1] + 2 * mem.shape[2]), jnp.float32),
        in_specs=[
            pl.BlockSpec(memory_space=pltpu.SMEM),
            pl.BlockSpec(memory_space=pltpu.VMEM),
            pl.BlockSpec(memory_space=pltpu.VMEM),
            pl.BlockSpec(memory_space=pltpu.VMEM),
        ],
        out_specs=pl.BlockSpec(memory_space=pltpu.VMEM),
        scratch_shapes=[
            pltpu.VMEM(rows.shape, rows.dtype),
        ],
        compiler_params=pltpu.CompilerParams(vmem_limit_bytes=16 * 2**20),
        name="base",
    )(turn, rows, ask, mem)


def shards(
    latest_activations,
    layer_normalizer_gains_table,
    asker_projection,
    memory_projection_stack,
    narrowing_factors,
    widening_factors_asker,
    widening_factors_memory,
    tweak_for_stream,
    stream_offsets,
    saved_rotated_addresses,
    saved_contents,
):
    n_bank = lax.axis_size("bank")
    n_tensor = lax.axis_size("tensor")
    bank_index = lax.axis_index("bank")
    tensor_index = lax.axis_index("tensor")
    row_count, piece_tensor = latest_activations.shape
    model_width = layer_normalizer_gains_table.shape[0]
    fold = n_bank // n_tensor

    own_float = latest_activations.astype(jnp.float32)
    part_square = jnp.sum(own_float * own_float, axis=1)
    square = sum(relative_blocks(part_square, "tensor", n_tensor))[:, None]
    tensor_gain = lax.dynamic_slice_in_dim(
        layer_normalizer_gains_table, tensor_index * piece_tensor, piece_tensor, 0
    )
    normed = (
        own_float
        * lax.rsqrt(square / model_width + epsilon)
        * tensor_gain.astype(jnp.float32)[None, :]
    ).astype(jnp.bfloat16)
    note = jnp.pad(digits_of(tweak_for_stream), ((0, 0), (0, 125)))
    package = jnp.concatenate([normed, note], axis=1)
    packages = jnp.concatenate(relative_blocks(package, "bank", n_bank), axis=0)
    hidden_after_rmsnorm = packages[:, :piece_tensor]
    all_ids = ids_from(packages[:, piece_tensor : piece_tensor + 3])
    base_rows = swapped(hidden_after_rmsnorm, n_bank, n_tensor, bank_index)
    source_bank = (bank_index % fold) * n_tensor + tensor_index
    turn = ((source_bank - bank_index) % n_bank) * (row_count // 8)

    sequences_on_device = narrowing_factors.shape[0]
    low_dim_extent = widening_factors_asker.shape[1]
    owned_ids = bank_index * sequences_on_device + jnp.arange(sequences_on_device, dtype=jnp.int32)
    picked = all_ids[None, :] == owned_ids[:, None]
    first = (bank_index * sequences_on_device).astype(jnp.int32)[None]
    inner_part, asker_staged, memory_staged = narrow(
        first,
        all_ids,
        hidden_after_rmsnorm,
        narrowing_factors,
        asker_projection,
        memory_projection_stack,
    )
    inner_sum = sum(relative_blocks(inner_part, "tensor", n_tensor))
    inner_low = inner_sum.astype(jnp.bfloat16)
    pick_low = picked.astype(jnp.bfloat16)
    base_part = base_product(turn.astype(jnp.int32)[None], base_rows, asker_staged, memory_staged)

    def spread(rank_block):
        expanded = pick_low[:, None, :] * rank_block[None, :, :]
        return expanded.reshape(sequences_on_device * low_dim_extent, rank_block.shape[1])

    probe_proj_span = asker_projection.shape[1]
    shared_proj_span = memory_projection_stack.shape[2]
    probe_correction = jnp.einsum(
        "cs,co->so",
        spread(inner_low[0:low_dim_extent]),
        widening_factors_asker.reshape(sequences_on_device * low_dim_extent, probe_proj_span),
        preferred_element_type=jnp.float32,
    )
    lookup_correction = jnp.einsum(
        "cs,co->so",
        spread(inner_low[low_dim_extent : 2 * low_dim_extent]),
        widening_factors_memory[:, 0].reshape(
            sequences_on_device * low_dim_extent, shared_proj_span
        ),
        preferred_element_type=jnp.float32,
    )
    payload_correction = jnp.einsum(
        "cs,co->so",
        spread(inner_low[2 * low_dim_extent : 3 * low_dim_extent]),
        widening_factors_memory[:, 1].reshape(
            sequences_on_device * low_dim_extent, shared_proj_span
        ),
        preferred_element_type=jnp.float32,
    )
    share = base_part + tweak_strength * jnp.concatenate(
        [probe_correction, lookup_correction, payload_correction], axis=1
    )
    accumulated_total = share[:row_count]
    for r in range(1, n_bank):
        accumulated_total = accumulated_total + lax.ppermute(
            share[r * row_count : (r + 1) * row_count], "bank", ring(n_bank, -r)
        )
    head_dim = saved_rotated_addresses.shape[3]
    kv_heads = saved_rotated_addresses.shape[2]
    q_heads = probe_proj_span // head_dim
    query_part = accumulated_total[:, 0:probe_proj_span].reshape(row_count, q_heads, head_dim)
    key_part = accumulated_total[:, probe_proj_span : probe_proj_span + shared_proj_span].reshape(
        row_count, kv_heads, head_dim
    )
    value_part = accumulated_total[
        :, probe_proj_span + shared_proj_span : probe_proj_span + 2 * shared_proj_span
    ].reshape(row_count, kv_heads, head_dim)
    q_rot = rotate(query_part, stream_offsets).astype(jnp.bfloat16)
    k_new = rotate(key_part, stream_offsets).astype(jnp.bfloat16)
    v_new = value_part.astype(jnp.bfloat16)
    probe_vectors = q_rot.reshape(row_count, kv_heads, q_heads // kv_heads, head_dim)
    mixed = attend_local(
        probe_vectors, k_new, v_new, saved_rotated_addresses, saved_contents, stream_offsets
    )
    return mixed.reshape(row_count, probe_proj_span).astype(jnp.bfloat16)


def solution(mesh):
    placed = (
        P(("groups", "bank"), "tensor"),
        P(),
        P("bank", "tensor"),
        P(None, "bank", "tensor"),
        P("bank", None, "tensor"),
        P("bank", None, "tensor"),
        P("bank", None, None, "tensor"),
        P(("groups", "bank")),
        P(("groups", "bank")),
        P(("groups", "bank"), None, "tensor", None),
        P(("groups", "bank"), None, "tensor", None),
    )

    return jax.shard_map(
        shards,
        mesh=mesh,
        in_specs=placed,
        out_specs=P(("groups", "bank"), "tensor"),
        check_vma=False,
    )
```
